128 devices in a mesh: dp: 128 (over y, x, z, core).
Axes of the slice: x: 4, y: 4, z: 4, core: 2. Of those that a mesh axis runs over, the one named last changes fastest.
Arguments:
- patches: bfloat16 [98304, 1280], P('dp'), may hold values from -6 to 6
- patch_grids: int32 [768, 4, 2], P('dp'), may hold values from 0 to 16, as said below
- block_counts: int32 [128], replicated, may hold values from 0 to 6, as said below
- send_counts: int32 [7, 128], replicated, may hold values from 0 to 2, as said below
- row_table: bfloat16 [16, 1280], replicated, may hold values from -3 to 3
- col_table: bfloat16 [16, 1280], replicated, may hold values from -3 to 3
- ln_gain: bfloat16 [1280], replicated, may hold values from 0.25 to 1.75
- ln_bias: bfloat16 [1280], replicated, may hold values from -3 to 3
- w_qkv: bfloat16 [1280, 1920], replicated, may hold values from -1.2 to 1.2
- b_qkv: bfloat16 [1920], replicated, may hold values from -3 to 3
- w_out: bfloat16 [640, 1280], replicated, may hold values from -0.25 to 0.25
- b_out: bfloat16 [1280], replicated, may hold values from -3 to 3
- cotangent: bfloat16 [65536, 1280], P('dp'), may hold values from -1.5 to 1.5
Outputs:
- block_output: bfloat16 [65536, 1280], P('dp')
- grad_w_qkv: float32 [1280, 1920], P('dp')
- grad_w_out: float32 [640, 1280], P('dp')
The draws below stay inside these ranges and needn't reach their ends.
Inputs may be any that keep to these rules, and one draw needn't show every extreme that they name: `patch_grids`: in each block slot the areas h * w of its 4 images sum to at most 128; heights are 1 to 16, widths 0 to 16, width 0 meaning no image. `block_counts`: live blocks of each rank at the start; with send_counts no rank holds more than 6 live blocks during balancing, and after the last section every rank holds 2 to 4, some rank exactly 4. `send_counts`: A rank never sends more blocks than it holds live; of two partners in a section at most one sends; in every draw some rank sends exactly 2 blocks in the last section.
All inputs are finite; a program needn't handle non-finite values.
Results may differ from the reference program's by a relative error of at most 0.0075.
Values may be sent and summed in bfloat16 or wider, within the bound.
No kernel may reach another device: no remote copies, remote signals or barrier semaphores. Data moves between devices by JAX's collectives and lax.ppermute only.
A program may use at most 128 MiB of HBM per device.

```python
import math
import jax
import jax.numpy as jnp
from jax import lax

D = 1280
HEAD = 80
HEADS = 8
BLOCK = 128
GRID = 16
IMGS = 4
BAL = 4
SLOTS = 6
MOVE = 2
SECTIONS = 7
TOKENS = 65536
DEVICES = 128


def balance_plan(key):
    base = jax.random.fold_in(key, 11)
    final_key = jax.random.fold_in(base, 1)
    chosen_key = jax.random.fold_in(base, 2)
    section_key = jax.random.fold_in(base, 3)
    all_ranks = jnp.arange(DEVICES, dtype=jnp.int32)
    counts = jax.random.randint(final_key, (DEVICES,), 2, BAL + 1).astype(jnp.int32)
    fullest = jax.random.randint(chosen_key, (), 0, DEVICES).astype(jnp.int32)
    counts = jnp.where(all_ranks == fullest, BAL, counts).astype(jnp.int32)
    sends = [None] * SECTIONS
    for section_index in reversed(range(SECTIONS)):
        bit_value = 1 << section_index
        partner = jnp.bitwise_xor(all_ranks, bit_value).astype(jnp.int32)
        lower = jnp.bitwise_and(all_ranks, bit_value) == 0
        after_own = counts
        after_other = counts[partner]
        total = after_own + after_other
        low_end = jnp.maximum(jnp.maximum(total - SLOTS, after_own - MOVE), 0)
        high_end = jnp.minimum(jnp.minimum(total, after_own + MOVE), SLOTS)
        raw_draw = jax.random.randint(jax.random.fold_in(section_key, section_index), (DEVICES,), 0, 1 << 20)
        picked = (low_end + raw_draw % (high_end - low_end + 1)).astype(jnp.int32)
        before = jnp.where(lower, picked, total - picked[partner]).astype(jnp.int32)
        if section_index == SECTIONS - 1:
            before = jnp.where(all_ranks == fullest, after_own - MOVE, before)
            before = jnp.where(partner == fullest, total - (after_other - MOVE), before).astype(jnp.int32)
        sends[section_index] = jnp.maximum(before - after_own, 0).astype(jnp.int32)
        counts = before
    return (counts, jnp.stack(sends, axis=0).astype(jnp.int32))


def draw_block_counts(key, part):
    return balance_plan(key)[0]


def draw_send_counts(key, part):
    return balance_plan(key)[1]


def draw_patch_grids(key, part):
    room_left = jnp.full((DEVICES * SLOTS,), BLOCK, jnp.int32)
    columns = []
    for image_slot in range(IMGS):
        height_draw = jax.random.randint(jax.random.fold_in(key, 2 * image_slot), (DEVICES * SLOTS,), 1, GRID + 1).astype(jnp.int32)
        width_draw = jax.random.randint(jax.random.fold_in(key, 2 * image_slot + 1), (DEVICES * SLOTS,), 1, GRID + 1).astype(jnp.int32)
        width_draw = jnp.minimum(width_draw, room_left // height_draw).astype(jnp.int32)
        room_left = (room_left - height_draw * width_draw).astype(jnp.int32)
        columns.append(jnp.stack([height_draw, width_draw], axis=-1))
    return jnp.stack(columns, axis=1).astype(jnp.int32)


def draw_w_qkv(key, part):
    inner = HEADS * HEAD
    values = jax.random.normal(key, (D, 3 * inner), jnp.float32) * (1.0 / D ** 0.5)
    return jnp.clip(values, -1.1953125, 1.1953125).astype(jnp.bfloat16)


def steps_of(key, extent, split, smallest, high):
    factor_of, own = 1.0, jax.random.fold_in(key, 6)
    for dim, blocks in split:
        steps = jnp.exp(jax.random.uniform(jax.random.fold_in(own, dim), (blocks,), jnp.float32, smallest / len(split), high / len(split)))
        factor_of = factor_of * jnp.repeat(steps, extent[dim] // blocks).reshape([-1 if axis == dim else 1 for axis in range(len(extent))])
    return factor_of


def scatter_about(own_key, dims, width, bound, shards=(), kind=jnp.bfloat16):
    values = width * jax.random.normal(own_key, dims, jnp.float32)
    if shards:
        values = values * steps_of(own_key, dims, shards, -0.22, 0.18)
    return jnp.clip(values, -bound, bound).astype(kind)


def setup_inputs(seed: int = 0) -> dict:
    key_of = jax.random.split(jax.random.key(seed), 14)
    return {
        "patches": scatter_about(key_of[0], (DEVICES * SLOTS * BLOCK, D), 1.0, 6.0, ((0, 128),)),
        "patch_grids": draw_patch_grids(jax.random.fold_in(key_of[13], 71), 0),
        "block_counts": draw_block_counts(jax.random.fold_in(key_of[13], 71), 0),
        "send_counts": draw_send_counts(jax.random.fold_in(key_of[13], 71), 0),
        "row_table": scatter_about(key_of[4], (GRID, D), 0.5, 3.0),
        "col_table": scatter_about(key_of[5], (GRID, D), 0.5, 3.0),
        "ln_gain": jnp.clip(1.0 + 0.15 * jax.random.normal(key_of[6], (D,), jnp.float32), 0.25, 1.75).astype(jnp.bfloat16),
        "ln_bias": scatter_about(key_of[7], (D,), 0.5, 3.0),
        "w_qkv": draw_w_qkv(jax.random.fold_in(key_of[13], 71), 0),
        "b_qkv": scatter_about(key_of[9], (3 * HEADS * HEAD,), 0.5, 3.0),
        "w_out": scatter_about(key_of[10], (HEADS * HEAD, D), (HEADS * HEAD) ** -0.5, 0.25),
        "b_out": scatter_about(key_of[11], (D,), 0.5, 3.0),
        "cotangent": scatter_about(key_of[12], (TOKENS, D), (24 * TOKENS ** -0.5), 1.5, ((0, 128),)),
    }


EPSILON = 1e-06

def token_layout(patch_grids):
    heights = patch_grids[:, :, 0]
    widths = patch_grids[:, :, 1]
    image_area = (heights * widths).astype(jnp.int32)
    image_end = jnp.cumsum(image_area, axis=1).astype(jnp.int32)
    image_start = (image_end - image_area).astype(jnp.int32)
    positions = jnp.arange(BLOCK, dtype=jnp.int32)[None, :, None]
    member = ((positions >= image_start[:, None, :]) & (positions < image_end[:, None, :])).astype(jnp.int32)
    image_ids = jnp.arange(patch_grids.shape[1], dtype=jnp.int32)
    in_image = lax.optimization_barrier(jnp.sum(member, axis=-1)).astype(jnp.int32)
    segment = (lax.optimization_barrier(jnp.sum(member * image_ids, axis=-1)).astype(jnp.int32) + in_image - 1).astype(jnp.int32)
    offset = (positions[:, :, 0] - lax.optimization_barrier(jnp.sum(member * image_start[:, None, :], axis=-1))).astype(jnp.int32)
    offset = offset * in_image
    span = jnp.maximum(lax.optimization_barrier(jnp.sum(member * widths[:, None, :], axis=-1)).astype(jnp.int32), 1)
    row_index = (offset // span).astype(jnp.int32)
    col_index = (offset - row_index * span).astype(jnp.int32)
    return (segment, row_index, col_index, in_image)

def embed_blocks(patch_rows, patch_grids, row_table, col_table):
    block_total = patch_grids.shape[0]
    segment, row_index, col_index, in_image = token_layout(patch_grids)
    levels = jnp.arange(row_table.shape[0], dtype=jnp.int32)
    row_hot = (row_index.reshape(-1, 1) == levels[None, :]).astype(jnp.bfloat16)
    col_hot = (col_index.reshape(-1, 1) == levels[None, :]).astype(jnp.bfloat16)
    table_sum = jnp.dot(row_hot, row_table, preferred_element_type=jnp.float32) + jnp.dot(col_hot, col_table, preferred_element_type=jnp.float32)
    embedded = (patch_rows.astype(jnp.float32) + table_sum * in_image.reshape(-1, 1).astype(jnp.float32)).astype(jnp.bfloat16)
    return (embedded.reshape(block_total, BLOCK, patch_rows.shape[1]), segment)

def layer_forward(blocks, marks, ln_gain, ln_bias, w_qkv, b_qkv, w_out, b_out):
    block_total = blocks.shape[0]
    model_width = blocks.shape[2]
    inner = w_out.shape[0]
    head_count = inner // HEAD
    rows = blocks.reshape(block_total * BLOCK, model_width).astype(jnp.float32)
    average = lax.optimization_barrier(jnp.mean(rows, axis=-1, keepdims=True))
    centred = rows - average
    variance = lax.optimization_barrier(jnp.mean(centred * centred, axis=-1, keepdims=True))
    normed = (centred * lax.rsqrt(variance + EPSILON) * ln_gain.astype(jnp.float32) + ln_bias.astype(jnp.float32)).astype(jnp.bfloat16)
    mixed = (jnp.dot(normed, w_qkv, preferred_element_type=jnp.float32) + b_qkv.astype(jnp.float32)).astype(jnp.bfloat16)
    shaped = mixed.reshape(block_total, BLOCK, 3, head_count, HEAD).astype(jnp.float32)
    query_f = shaped[:, :, 0]
    key_f = shaped[:, :, 1]
    value_f = shaped[:, :, 2]
    score_scale = 1.0 / math.sqrt(HEAD)
    scores = jnp.einsum('bqhd,bkhd->bhqk', query_f, key_f) * score_scale
    same_image = marks[:, :, None] == marks[:, None, :]
    scores = jnp.where(same_image[:, None], scores, -1e+30)
    top_score = lax.optimization_barrier(jnp.max(scores, axis=-1, keepdims=True))
    expo = jnp.exp(scores - top_score)
    probs_f = expo / lax.optimization_barrier(jnp.sum(expo, axis=-1, keepdims=True))
    probs_b = probs_f.astype(jnp.bfloat16)
    attended = jnp.einsum('bhqk,bkhd->bqhd', probs_b.astype(jnp.float32), value_f)
    attended = attended.reshape(block_total * BLOCK, inner).astype(jnp.bfloat16)
    projected = jnp.dot(attended, w_out, preferred_element_type=jnp.float32) + b_out.astype(jnp.float32)
    result = (rows + projected).astype(jnp.bfloat16)
    return (result, (normed, query_f, key_f, value_f, probs_f, probs_b, attended))

def output_backward(out_grad, saved, w_out):
    normed, query_f, key_f, value_f, probs_f, probs_b, attended = saved
    grad_out = jnp.dot(attended.T, out_grad, preferred_element_type=jnp.float32)
    attn_grad = jnp.dot(out_grad, w_out.T, preferred_element_type=jnp.float32)
    return (grad_out, attn_grad.reshape(query_f.shape))

def qkv_backward(attn_grad, saved):
    normed, query_f, key_f, value_f, probs_f, probs_b, attended = saved
    score_scale = 1.0 / math.sqrt(HEAD)
    prob_grad = jnp.einsum('bqhd,bkhd->bhqk', attn_grad, value_f)
    value_grad = jnp.einsum('bhqk,bqhd->bkhd', probs_b.astype(jnp.float32), attn_grad)
    score_grad = probs_f * (prob_grad - lax.optimization_barrier(jnp.sum(prob_grad * probs_f, axis=-1, keepdims=True))) * score_scale
    query_grad = jnp.einsum('bhqk,bkhd->bqhd', score_grad, key_f)
    key_grad = jnp.einsum('bhqk,bqhd->bkhd', score_grad, query_f)
    row_total = query_f.shape[0] * query_f.shape[1]
    mixed_grad = jnp.stack([query_grad, key_grad, value_grad], axis=2).reshape(row_total, -1).astype(jnp.bfloat16)
    return jnp.dot(normed.T, mixed_grad, preferred_element_type=jnp.float32)

def balance_anchor(block_counts, send_counts):
    all_ranks = jnp.arange(DEVICES, dtype=jnp.int32)
    slot_ids = jnp.arange(SLOTS, dtype=jnp.int32)[None, :]
    anchor = (all_ranks[:, None] * SLOTS + slot_ids).astype(jnp.int32)
    counts = block_counts.astype(jnp.int32)
    for section_index in range(SECTIONS):
        partner = jnp.bitwise_xor(all_ranks, 1 << section_index).astype(jnp.int32)
        sent_now = send_counts[section_index].astype(jnp.int32)
        received = sent_now[partner]
        their_count = counts[partner]
        staying = slot_ids < (counts - sent_now)[:, None]
        landing = (slot_ids >= counts[:, None]) & (slot_ids < (counts + received)[:, None])
        source = jnp.clip(their_count[:, None] - received[:, None] + slot_ids - counts[:, None], 0, SLOTS - 1).astype(jnp.int32)
        incoming = anchor[partner[:, None], source]
        anchor = jnp.where(staying, anchor, jnp.where(landing, incoming, 0)).astype(jnp.int32)
        counts = (counts - sent_now + received).astype(jnp.int32)
    return (anchor, counts)

def reference(patches, patch_grids, block_counts, send_counts, row_table, col_table, ln_gain, ln_bias, w_qkv, b_qkv, w_out, b_out, cotangent):
    model_width = patches.shape[1]
    embedded, segment = embed_blocks(patches, patch_grids, row_table, col_table)
    anchor, counts = balance_anchor(block_counts, send_counts)
    chosen = anchor[:, :BAL].astype(jnp.int32)
    live = jnp.arange(BAL, dtype=jnp.int32)[None, :] < counts[:, None]
    blocks = embedded[chosen]
    marks = segment[chosen].astype(jnp.float32)
    rank_grads = cotangent.reshape(DEVICES, BAL * BLOCK, model_width)

    def one_rank(carry, inputs):
        rank_blocks, rank_marks, rank_live, rank_cot = inputs
        result, saved = layer_forward(rank_blocks, rank_marks, ln_gain, ln_bias, w_qkv, b_qkv, w_out, b_out)
        token_live = (rank_live[:, None] & (rank_marks >= 0)).reshape(-1, 1)
        out_grad = jnp.where(token_live, rank_cot, jnp.zeros_like(rank_cot)).astype(jnp.bfloat16)
        grad_out, attn_grad = output_backward(out_grad, saved, w_out)
        grad_qkv = qkv_backward(attn_grad, saved)
        slot_live = jnp.repeat(rank_live, BLOCK).reshape(-1, 1)
        result = jnp.where(slot_live, result, jnp.zeros_like(result))
        return ((carry[0] + grad_qkv, carry[1] + grad_out), result)
    start = (jnp.zeros(w_qkv.shape, jnp.float32), jnp.zeros(w_out.shape, jnp.float32))
    totals, outputs = lax.scan(one_rank, start, (blocks, marks, live, rank_grads))
    return (outputs.reshape(TOKENS, model_width), totals[0], totals[1])
```

```python
import functools
import math

import jax
import jax.numpy as jnp
from jax import lax
from jax.experimental import pallas as pl
from jax.experimental.pallas import tpu as pltpu
from jax.sharding import PartitionSpec as P

HEAD = 80
BLOCK = 128
EPSILON = 1e-06
AXIS = "dp"

MARK = 8
PIECES = (56, 72)
STACK = 8
WINDOW = 2
GROUPS = ((0,), (1, 2), (3, 4), (5, 6))
FIELDS = 8

SMEM = pl.BlockSpec(memory_space=pltpu.SMEM)
VMEM = pl.BlockSpec(memory_space=pltpu.VMEM)


def payload_rows(piece):
    return PIECES[piece] + (MARK if piece == 0 else 0)


def masks_of(group):
    first = 1 << GROUPS[group][0]
    if len(GROUPS[group]) == 1:
        return (first,)
    second = 1 << GROUPS[group][1]
    return (first, second, first ^ second)


def exchange(values, group):
    size = lax.axis_size(AXIS)
    return [
        lax.ppermute(value, AXIS, [(i, i ^ mask) for i in range(size)])
        for value, mask in zip(values, masks_of(group))
    ]


def plan_kernel(counts_ref, sends_ref, table_ref):
    me = lax.axis_index(AXIS)
    count = counts_ref[me]
    for group, sections in enumerate(GROUPS):
        first = 1 << sections[0]
        m_a = sends_ref[sections[0], me]
        n_a = sends_ref[sections[0], me ^ first]
        if len(sections) == 1:
            values = (count - m_a, 0, 0, count, n_a, count - m_a + n_a, 0, 0)
            after = count - m_a + n_a
        else:
            second = 1 << sections[1]
            m_b = sends_ref[sections[1], me]
            n_b = sends_ref[sections[1], me ^ second]
            passed_on = jnp.minimum(sends_ref[sections[1], me ^ first], m_a)
            forwarded = jnp.minimum(n_b, sends_ref[sections[0], me ^ first ^ second])
            floor = count - m_a + n_a - m_b
            values = (
                count - m_a,
                count - m_a - (m_b - jnp.minimum(m_b, n_a)),
                count - passed_on,
                count,
                jnp.clip(floor - count, 0, n_a),
                floor,
                n_b - forwarded,
                forwarded,
            )
            after = floor + n_b
        for field, value in enumerate(values):
            table_ref[group * FIELDS + field] = jnp.int32(value)
        count = after
    table_ref[len(GROUPS) * FIELDS] = count


def make_plan(block_counts, send_counts):
    return pl.pallas_call(
        plan_kernel,
        out_shape=jax.ShapeDtypeStruct((len(GROUPS) * FIELDS + 8,), jnp.int32),
        in_specs=[SMEM, SMEM],
        out_specs=SMEM,
        name="plan",
    )(block_counts, send_counts)


def cut(table_ref, stack_ref, window_refs, group):
    for which, window_ref in enumerate(window_refs):
        low = table_ref[group * FIELDS + which]
        for i in range(WINDOW):
            window_ref[i] = stack_ref[low + i]


def land(table_ref, stack_ref, far_refs, group):
    base = group * FIELDS
    floor = table_ref[base + 5]
    targets = (
        (table_ref[base + 3], table_ref[base + 4]),
        (floor, table_ref[base + 6]),
        (floor + table_ref[base + 6], table_ref[base + 7]),
    )
    for far_ref, (start, total) in zip(far_refs, targets):
        for i in range(WINDOW):

            @pl.when(i < total)
            def _():
                stack_ref[start + i] = far_ref[i]


def open_kernel(piece, begin, table_ref, patches_ref, *rest):
    if piece == 0:
        grids_ref, stack_ref, window_ref, sem = rest
    else:
        stack_ref, window_ref, sem = rest
    rows = PIECES[piece]
    slots = patches_ref.shape[0]
    copy = pltpu.make_async_copy(
        patches_ref.at[:, pl.ds(begin, rows)], stack_ref.at[pl.ds(0, slots), pl.ds(0, rows)], sem
    )
    copy.start()
    for slot in range(slots, STACK):
        stack_ref[slot] = jnp.zeros(stack_ref.shape[1:], stack_ref.dtype)
    if piece == 0:
        for slot in range(slots):
            stack_ref[slot, rows:, :] = grids_ref[slot]
    copy.wait()
    cut(table_ref, stack_ref, (window_ref,), 0)


def open_piece(table, patches, grids, piece):
    rows = payload_rows(piece)
    width = patches.shape[-1]
    begin = sum(PIECES[:piece])
    extra = (grids,) if piece == 0 else ()
    return pl.pallas_call(
        functools.partial(open_kernel, piece, begin),
        out_shape=(
            jax.ShapeDtypeStruct((STACK, rows, width), patches.dtype),
            jax.ShapeDtypeStruct((WINDOW, rows, width), patches.dtype),
        ),
        in_specs=[SMEM, pl.BlockSpec(memory_space=pl.ANY)] + [VMEM] * len(extra),
        out_specs=(VMEM, VMEM),
        scratch_shapes=[pltpu.SemaphoreType.DMA],
        name=f"open_{piece}",
    )(table, patches, *extra)


def turn_kernel(group, table_ref, old_ref, *rest):
    far_count = len(masks_of(group))
    fars = rest[:far_count]
    stack_ref = rest[far_count]
    windows = rest[far_count + 1 :]
    stack_ref[...] = old_ref[: stack_ref.shape[0]]
    land(table_ref, stack_ref, fars, group)
    if windows:
        cut(table_ref, stack_ref, windows, group + 1)


def turn(table, stack, fars, group, piece, balanced):
    last = group == len(GROUPS) - 1
    slots = balanced if last else STACK
    window = jax.ShapeDtypeStruct((WINDOW,) + stack.shape[1:], stack.dtype)
    sends = 0 if last else len(masks_of(group + 1))
    out = pl.pallas_call(
        functools.partial(turn_kernel, group),
        out_shape=(jax.ShapeDtypeStruct((slots,) + stack.shape[1:], stack.dtype),) + (window,) * sends,
        in_specs=[SMEM, VMEM] + [VMEM] * len(fars),
        out_specs=(VMEM,) * (1 + sends),
        name=f"turn_{group}_{piece}",
    )(table, stack, *fars)
    return out[0], list(out[1:])


def balance(patches, patch_grids, table, balanced):
    slots = patch_grids.shape[0]
    width = patches.shape[-1]
    blocks = patches.reshape(slots, BLOCK, width)
    grids = jnp.broadcast_to(
        jnp.pad(
            patch_grids.reshape(slots, 1, -1).astype(jnp.bfloat16),
            ((0, 0), (0, 0), (0, width - patch_grids[0].size)),
        ),
        (slots, MARK, width),
    )
    stacks, windows = [], []
    for piece in range(len(PIECES)):
        stack, window = open_piece(table, blocks, grids, piece)
        stacks.append(stack)
        windows.append([window])
    for group in range(len(GROUPS)):
        for piece in range(len(PIECES)):
            fars = exchange(windows[piece], group)
            stacks[piece], windows[piece] = turn(
                table, stacks[piece], fars, group, piece, balanced
            )
    return stacks


def dot_nt(a, b):
    return lax.dot_general(a, b, (((1,), (1,)), ((), ())), preferred_element_type=jnp.float32)


def dot_tn(a, b):
    return lax.dot_general(a, b, (((0,), (0,)), ((), ())), preferred_element_type=jnp.float32)


def dot_nn(a, b):
    return lax.dot_general(a, b, (((1,), (0,)), ((), ())), preferred_element_type=jnp.float32)


def image_of_tokens(grid, positions):
    images = grid.shape[1] // 2
    zero = jnp.zeros_like(positions)
    segment, first, span, inside = zero - 1.0, zero, zero + 1.0, zero
    start = jnp.zeros((1, 1), jnp.float32)
    for j in range(images):
        width = grid[:, 2 * j + 1 : 2 * j + 2]
        end = start + grid[:, 2 * j : 2 * j + 1] * width
        member = (positions >= start) & (positions < end)
        segment = jnp.where(member, float(j), segment)
        first = jnp.where(member, start, first)
        span = jnp.where(member, width, span)
        inside = jnp.where(member, 1.0, inside)
        start = end
    offset = (positions - first) * inside
    row = jnp.floor((offset + 0.5) / span)
    return segment, row, offset - row * span, inside


def layer_kernel(
    table_ref,
    *refs,
):
    pieces = len(PIECES)
    stack_refs = refs[:pieces]
    (
        levels_ref,
        gain_ref,
        bias_ref,
        wall_hbm,
        ball_ref,
        w_out_hbm,
        turn_out_ref,
        b_out_ref,
        cot_hbm,
        result_ref,
        given_ref,
        kept_ref,
        x_ref,
        normed_ref,
        mixed_ref,
        grad_ref,
        attended_ref,
        out_grad_ref,
        attn_grad_ref,
        lines_ref,
        seg_row_ref,
        seg_col_ref,
        wall_ref,
        w_out_ref,
        cot_ref,
        sems,
    ) = refs[pieces:]
    balanced = stack_refs[0].shape[0]
    width = x_ref.shape[1]
    tokens = balanced * BLOCK
    inner = w_out_ref.shape[0]
    heads = inner // HEAD
    live_count = table_ref[len(GROUPS) * FIELDS]
    images = 4
    copies = [
        pltpu.make_async_copy(src, dst, sems.at[i])
        for i, (src, dst) in enumerate(
            ((cot_hbm, cot_ref), (w_out_hbm, w_out_ref), (wall_hbm, wall_ref))
        )
    ]
    for copy in copies:
        copy.start()

    col = lax.broadcasted_iota(jnp.int32, (BLOCK, 1), 0).astype(jnp.float32)
    lane = lax.broadcasted_iota(jnp.int32, (1, BLOCK), 1).astype(jnp.float32)
    level = lax.broadcasted_iota(jnp.int32, (BLOCK, levels_ref.shape[0]), 1).astype(jnp.float32)
    half = float(levels_ref.shape[0] // 2)

    for slot in range(balanced):
        at = slot * BLOCK
        grid = stack_refs[0][slot, PIECES[0] : PIECES[0] + MARK, :BLOCK].astype(jnp.float32)
        grid = grid[0:1, : 2 * images]
        segment, row, column, inside = image_of_tokens(grid, col)
        seg_col_ref[at : at + BLOCK, :] = segment
        seg_row_ref[slot] = jnp.broadcast_to(
            image_of_tokens(grid, lane)[0], (8, BLOCK)
        )
        hot = jnp.where((level == row) | (level == column + half), inside, 0.0)
        emb = dot_nn(hot.astype(jnp.bfloat16), levels_ref[...])
        begin = 0
        for piece, rows in enumerate(PIECES):
            raw = stack_refs[piece][slot, :rows, :].astype(jnp.float32)
            x_ref[at + begin : at + begin + rows, :] = (
                raw + emb[begin : begin + rows, :]
            ).astype(jnp.bfloat16)
            begin += rows
        rows = x_ref[at : at + BLOCK, :].astype(jnp.float32)
        centred = rows - jnp.sum(rows, axis=1, keepdims=True) * (1.0 / width)
        variance = jnp.sum(centred * centred, axis=1, keepdims=True) * (1.0 / width)
        normed_ref[at : at + BLOCK, :] = (
            centred * lax.rsqrt(variance + EPSILON) * gain_ref[...] + bias_ref[...]
        ).astype(jnp.bfloat16)

    copies[0].wait()
    for slot in range(balanced):
        at = slot * BLOCK
        keep = (seg_col_ref[at : at + BLOCK, :] >= 0.0) & (slot < live_count)
        out_grad_ref[at : at + BLOCK, :] = jnp.where(
            keep, cot_ref[at : at + BLOCK, :].astype(jnp.float32), 0.0
        ).astype(jnp.bfloat16)
    copies[1].wait()
    attn_grad_ref[...] = dot_nt(w_out_ref[...], out_grad_ref[...]).astype(jnp.bfloat16)
    copies[2].wait()
    step = 640
    for at in range(0, wall_ref.shape[0], step):
        mixed_ref[at : at + step, :] = (
            dot_nt(wall_ref[at : at + step, :], normed_ref[...]) + ball_ref[at : at + step, :]
        ).astype(jnp.bfloat16)

    scale = 1.0 / math.sqrt(HEAD)

    def one_slot(slot, carry):
        at = pl.multiple_of(slot * BLOCK, BLOCK)
        span = pl.ds(at, BLOCK)
        same = seg_col_ref[span, :] == seg_row_ref[slot, 0:1, :]
        for head in range(heads):
            h = head * HEAD
            query = mixed_ref[h : h + HEAD, span]
            key = mixed_ref[inner + h : inner + h + HEAD, span]
            value = mixed_ref[2 * inner + h : 2 * inner + h + HEAD, span]
            attn_grad = attn_grad_ref[h : h + HEAD, span]
            scores = jnp.where(same, dot_tn(key, query) * scale, -1e30)
            expo = jnp.exp(scores - jnp.max(scores, axis=0, keepdims=True))
            probs = expo * (1.0 / jnp.sum(expo, axis=0, keepdims=True))
            probs_b = probs.astype(jnp.bfloat16)
            attended_ref[h : h + HEAD, span] = dot_nn(value, probs_b).astype(jnp.bfloat16)
            prob_grad = dot_tn(value, attn_grad)
            grad_ref[2 * inner + h : 2 * inner + h + HEAD, span] = dot_nt(
                attn_grad, probs_b
            ).astype(jnp.bfloat16)
            mean = jnp.sum(prob_grad * probs, axis=0, keepdims=True)
            score_grad = (probs * (prob_grad - mean) * scale).astype(jnp.bfloat16)
            grad_ref[h : h + HEAD, span] = dot_nn(key, score_grad).astype(jnp.bfloat16)
            grad_ref[inner + h : inner + h + HEAD, span] = dot_nt(query, score_grad).astype(
                jnp.bfloat16
            )
        return carry

    lax.fori_loop(0, balanced, one_slot, 0)

    for slot in range(balanced):
        at = slot * BLOCK
        projected = dot_tn(attended_ref[:, at : at + BLOCK], w_out_ref[...]) + b_out_ref[...]
        total = x_ref[at : at + BLOCK, :].astype(jnp.float32) + projected
        result_ref[at : at + BLOCK, :] = jnp.where(slot < live_count, total, 0.0).astype(
            jnp.bfloat16
        )

    turned = dot_nn(turn_out_ref[...], attended_ref[...]).astype(jnp.bfloat16)
    chips = given_ref.shape[0]
    qkv_tiles = 3 * inner // 128
    out_tiles = width // 128
    per_rank = width // (2 * chips)
    out_rank = inner // (2 * chips)
    base = 3 * inner
    even = 8 * chips
    for part, target in enumerate((given_ref, kept_ref)):
        row = base + part * per_rank * chips
        eights = mixed_ref[row : row + even, :]
        others = mixed_ref[row + even : row + per_rank * chips, :]
        rest = per_rank - 8
        group = 3
        for tile in range(0, qkv_tiles, group):
            piece = grad_ref[tile * 128 : (tile + group) * 128, :]
            block = dot_nt(eights, piece).astype(jnp.bfloat16)
            side = dot_nt(others, piece)
            for t in range(group):
                target[:, 8 * (tile + t) : 8 * (tile + t) + 8, :] = block[
                    :, t * 128 : (t + 1) * 128
                ].reshape(chips, 8, 128)
                for e in range(rest):
                    line = ((tile + t) * rest + e) * chips
                    lines_ref[line : line + chips, :] = side[
                        e * chips : (e + 1) * chips, t * 128 : (t + 1) * 128
                    ]
        block = dot_nn(turned[part * out_rank * chips : (part + 1) * out_rank * chips, :], out_grad_ref[...])
        for t in range(out_tiles):
            for e in range(out_rank):
                line = (qkv_tiles * rest + t * out_rank + e) * chips
                lines_ref[line : line + chips, :] = block[
                    e * chips : (e + 1) * chips, t * 128 : (t + 1) * 128
                ]
        count = qkv_tiles * rest + out_tiles * out_rank

        def one_chip(chip, carry):
            for b in range(count // 8):
                lines = lines_ref[pl.ds(chip + b * 8 * chips, 8, stride=chips), :]
                target[chip, 8 * qkv_tiles + 8 * b : 8 * qkv_tiles + 8 * b + 8, :] = lines.astype(
                    jnp.bfloat16
                )
            return carry

        lax.fori_loop(0, chips, one_chip, 0)


def layer(table, stacks, levels, gain, bias, wall, ball, w_out, turn_out, b_out, cotangent):
    width = cotangent.shape[1]
    tokens = cotangent.shape[0]
    balanced = tokens // BLOCK
    inner = w_out.shape[0]
    chips = lax.axis_size(AXIS) // 2
    lines = (width // (2 * chips) * 3 * inner + inner // (2 * chips) * width) // 128
    any_space = pl.BlockSpec(memory_space=pl.ANY)
    first = [VMEM] * len(stacks)
    bf16, f32 = jnp.bfloat16, jnp.float32
    return pl.pallas_call(
        layer_kernel,
        out_shape=(
            jax.ShapeDtypeStruct((tokens, width), bf16),
            jax.ShapeDtypeStruct((chips, lines, 128), bf16),
            jax.ShapeDtypeStruct((chips, lines, 128), bf16),
        ),
        in_specs=[SMEM]
        + first
        + [VMEM, VMEM, VMEM, any_space, VMEM, any_space, VMEM, VMEM, any_space],
        out_specs=(VMEM, VMEM, VMEM),
        scratch_shapes=[
            pltpu.VMEM((tokens, width), bf16),
            pltpu.VMEM((tokens, width), bf16),
            pltpu.VMEM((wall.shape[0], tokens), bf16),
            pltpu.VMEM((3 * inner, tokens), bf16),
            pltpu.VMEM((inner, tokens), bf16),
            pltpu.VMEM((tokens, width), bf16),
            pltpu.VMEM((inner, tokens), bf16),
            pltpu.VMEM(((lines - 8 * (3 * inner // 128)) * chips, 128), f32),
            pltpu.VMEM((balanced, 8, BLOCK), f32),
            pltpu.VMEM((tokens, 1), f32),
            pltpu.VMEM(wall.shape, bf16),
            pltpu.VMEM(w_out.shape, bf16),
            pltpu.VMEM(cotangent.shape, bf16),
            pltpu.SemaphoreType.DMA((3,)),
        ],
        compiler_params=pltpu.CompilerParams(vmem_limit_bytes=60 * 1024 * 1024),
        name="layer",
    )(table, *stacks, levels, gain, bias, wall, ball, w_out, turn_out, b_out, cotangent)


def row_orders(width, inner):
    size = lax.axis_size(AXIS)
    chips = size // 2
    core = lax.axis_index(AXIS) & 1
    cores = jnp.stack([1 - core, core]).astype(jnp.int32)
    chip = jnp.arange(chips, dtype=jnp.int32)
    per, out = width // size, inner // size
    owner = (2 * chip[None, :] + cores[:, None]) * per
    eights = (owner[:, :, None] + jnp.arange(8, dtype=jnp.int32)).reshape(2, -1)
    others = (owner[:, None, :] + jnp.arange(8, per, dtype=jnp.int32)[None, :, None]).reshape(2, -1)
    qkv = jnp.concatenate([eights, others], axis=1).reshape(-1)
    owner = (2 * chip[None, :] + cores[:, None]) * out
    outs = (owner[:, None, :] + jnp.arange(out, dtype=jnp.int32)[None, :, None]).reshape(-1)
    return qkv, outs


def hot_rows(order):
    size = order.shape[0]
    return (order[:, None] == jnp.arange(size, dtype=jnp.int32)[None, :]).astype(jnp.bfloat16)


def chips_with_my_core(size):
    return [[2 * chip + core for chip in range(size // 2)] for core in range(2)]


def spread(given, kept, width, inner):
    size = lax.axis_size(AXIS)
    taken = lax.ppermute(given, AXIS, [(i, i ^ 1) for i in range(size)])
    pair = (kept.astype(jnp.float32) + taken.astype(jnp.float32)).astype(jnp.bfloat16)
    parts = lax.all_to_all(
        pair, AXIS, 0, 0, axis_index_groups=chips_with_my_core(size), tiled=True
    )
    total = jnp.sum(parts.astype(jnp.float32), axis=0)
    tiles, rest, out = 3 * inner // 128, width // size - 8, inner // size
    cuts = (8 * tiles, (8 + rest) * tiles)
    eights = total[: cuts[0]].reshape(tiles, 8, 128).transpose(1, 0, 2).reshape(8, -1)
    others = total[cuts[0] : cuts[1]].reshape(tiles, rest, 128).transpose(1, 0, 2).reshape(rest, -1)
    outs = total[cuts[1] :].reshape(width // 128, out, 128).transpose(1, 0, 2).reshape(out, -1)
    return jnp.concatenate([eights, others], axis=0), outs


def local(
    patches,
    patch_grids,
    block_counts,
    send_counts,
    row_table,
    col_table,
    ln_gain,
    ln_bias,
    w_qkv,
    b_qkv,
    w_out,
    b_out,
    cotangent,
):
    width, inner = cotangent.shape[1], w_out.shape[0]
    table = make_plan(block_counts, send_counts)
    qkv_order, out_order = row_orders(width, inner)
    wall = jnp.concatenate([w_qkv.T, hot_rows(qkv_order)], axis=0)
    ball = jnp.pad(b_qkv.astype(jnp.float32), (0, width)).reshape(-1, 1)
    stacks = balance(patches, patch_grids, table, cotangent.shape[0] // BLOCK)
    result, given, kept = layer(
        table,
        stacks,
        jnp.concatenate([row_table, col_table], axis=0),
        ln_gain.astype(jnp.float32).reshape(1, -1),
        ln_bias.astype(jnp.float32).reshape(1, -1),
        wall,
        ball,
        w_out,
        hot_rows(out_order),
        b_out.astype(jnp.float32).reshape(1, -1),
        cotangent,
    )
    qkv_rows, out_rows = spread(given, kept, width, inner)
    return (result, qkv_rows, out_rows)


def solution(mesh):
    return jax.shard_map(
        local,
        mesh=mesh,
        in_specs=(
            P("dp", None),
            P("dp", None, None),
            P(),
            P(),
            P(),
            P(),
            P(),
            P(),
            P(),
            P(),
            P(),
            P(),
            P("dp", None),
        ),
        out_specs=(P("dp", None), P("dp", None), P("dp", None)),
        check_vma=False,
    )
```

```python
import functools
import math

import jax
import jax.numpy as jnp
from jax import lax
from jax.experimental import pallas as pl
from jax.experimental.pallas import tpu as pltpu
from jax.sharding import PartitionSpec as P


HEAD = 80
BLOCK = 128
EPSILON = 1e-06
AXIS = "dp"

MARK = 8
PIECES = (56, 72)
STACK = 8
WINDOW = 2
GROUPS = ((0,), (1, 2), (3, 4), (5, 6))
FIELDS = 8
PAD = 4
SMALL = 10 * 1024 * 1024

SMEM = pl.BlockSpec(memory_space=pltpu.SMEM)
VMEM = pl.BlockSpec(memory_space=pltpu.VMEM)


def payload_rows(piece):
    return PIECES[piece] + (MARK if piece == 0 else 0)


def masks_of(group):
    first = 1 << GROUPS[group][0]
    if len(GROUPS[group]) == 1:
        return (first,)
    second = 1 << GROUPS[group][1]
    return (first, second, first ^ second)


def exchange(values, group):
    size = lax.axis_size(AXIS)
    out = []
    for value, mask in zip(values, masks_of(group)):
        out.append(lax.ppermute(value, AXIS, [(i, i ^ mask) for i in range(size)]))
    return out


def plan(counts_ref, sends_ref, table_ref):
    me = lax.axis_index(AXIS)
    count = counts_ref[me]
    for group, sections in enumerate(GROUPS):
        first = 1 << sections[0]
        m_a = sends_ref[sections[0], me]
        n_a = sends_ref[sections[0], me ^ first]
        if len(sections) == 1:
            values = (count - m_a, 0, 0, count, n_a, count - m_a + n_a, 0, 0)
            after = count - m_a + n_a
        else:
            second = 1 << sections[1]
            m_b = sends_ref[sections[1], me]
            n_b = sends_ref[sections[1], me ^ second]
            passed_on = jnp.minimum(sends_ref[sections[1], me ^ first], m_a)
            forwarded = jnp.minimum(n_b, sends_ref[sections[0], me ^ first ^ second])
            floor = count - m_a + n_a - m_b
            values = (
                count - m_a,
                count - m_a - (m_b - jnp.minimum(m_b, n_a)),
                count - passed_on,
                count,
                jnp.clip(floor - count, 0, n_a),
                floor,
                n_b - forwarded,
                forwarded,
            )
            after = floor + n_b
        for field, value in enumerate(values):
            table_ref[group * FIELDS + field] = jnp.int32(value)
        count = after
    table_ref[len(GROUPS) * FIELDS] = count


def cut(table_ref, stack_ref, window_refs, group):
    for which, window_ref in enumerate(window_refs):
        low = table_ref[group * FIELDS + which]
        for i in range(WINDOW):
            window_ref[i] = stack_ref[low + i]


def landings(table_ref, group):
    base = group * FIELDS
    floor = table_ref[base + 5]
    return (
        (table_ref[base + 3], table_ref[base + 4]),
        (floor, table_ref[base + 6]),
        (floor + table_ref[base + 6], table_ref[base + 7]),
    )


def land(table_ref, stack_ref, far_refs, group):
    for far_ref, (start, total) in zip(far_refs, landings(table_ref, group)):
        for i in range(WINDOW):

            @pl.when(i < total)
            def _():
                stack_ref[start + i] = far_ref[i]


def open_kernel(counts_ref, sends_ref, grids_ref, patches_ref, table_ref, *rest):
    pieces = len(PIECES)
    stack_refs, window_refs, sems = rest[:pieces], rest[pieces : 2 * pieces], rest[2 * pieces]
    slots = patches_ref.shape[0]
    copies, begin = [], 0
    for piece, rows in enumerate(PIECES):
        copies.append(
            pltpu.make_async_copy(
                patches_ref.at[:, pl.ds(begin, rows)],
                stack_refs[piece].at[pl.ds(0, slots), pl.ds(0, rows)],
                sems.at[piece],
            )
        )
        copies[-1].start()
        begin += rows
    plan(counts_ref, sends_ref, table_ref)
    for stack_ref in stack_refs:
        for slot in range(slots, STACK):
            stack_ref[slot] = jnp.zeros(stack_ref.shape[1:], stack_ref.dtype)
    numbers = grids_ref.shape[1] * grids_ref.shape[2]
    lane = lax.broadcasted_iota(jnp.int32, (MARK, 128), 1)
    for slot in range(slots):
        marks = jnp.zeros((MARK, 128), jnp.float32)
        for k in range(numbers):
            number = grids_ref[slot, k // 2, k % 2].astype(jnp.float32)
            marks = jnp.where(lane == k, number, marks)
        stack_refs[0][slot, PIECES[0] :, :128] = marks.astype(jnp.bfloat16)
        stack_refs[0][slot, PIECES[0] :, 128:] = jnp.zeros(
            (MARK, stack_refs[0].shape[2] - 128), jnp.bfloat16
        )
    for piece in range(pieces):
        copies[piece].wait()
        cut(table_ref, stack_refs[piece], (window_refs[piece],), 0)


def open_pieces(block_counts, send_counts, patch_grids, patches):
    width = patches.shape[-1]
    heights = [payload_rows(piece) for piece in range(len(PIECES))]
    out = pl.pallas_call(
        open_kernel,
        out_shape=(jax.ShapeDtypeStruct((len(GROUPS) * FIELDS + 8,), jnp.int32),)
        + tuple(jax.ShapeDtypeStruct((STACK, rows, width), patches.dtype) for rows in heights)
        + tuple(jax.ShapeDtypeStruct((WINDOW, rows, width), patches.dtype) for rows in heights),
        in_specs=[SMEM, SMEM, SMEM, pl.BlockSpec(memory_space=pltpu.HBM)],
        out_specs=(SMEM,) + (VMEM,) * (2 * len(PIECES)),
        scratch_shapes=[pltpu.SemaphoreType.DMA((len(PIECES),))],
        compiler_params=pltpu.CompilerParams(vmem_limit_bytes=SMALL),
        name="open",
    )(block_counts, send_counts, patch_grids, patches)
    count = len(PIECES)
    return out[0], list(out[1 : 1 + count]), [[window] for window in out[1 + count :]]


def turn_kernel(group, table_ref, old_ref, *rest):
    far_count = len(masks_of(group))
    fars = rest[:far_count]
    stack_ref = rest[far_count]
    windows = rest[far_count + 1 :]
    stack_ref[...] = old_ref[...]
    land(table_ref, stack_ref, fars, group)
    cut(table_ref, stack_ref, windows, group + 1)


def turn(table, stack, fars, group):
    window = jax.ShapeDtypeStruct((WINDOW,) + stack.shape[1:], stack.dtype)
    sends = len(masks_of(group + 1))
    out = pl.pallas_call(
        functools.partial(turn_kernel, group),
        out_shape=(jax.ShapeDtypeStruct(stack.shape, stack.dtype),) + (window,) * sends,
        in_specs=[SMEM, VMEM] + [VMEM] * len(fars),
        out_specs=(VMEM,) * (1 + sends),
        compiler_params=pltpu.CompilerParams(vmem_limit_bytes=SMALL),
    )(table, stack, *fars)
    return out[0], list(out[1:])


def balance(patches, patch_grids, block_counts, send_counts):
    slots = patch_grids.shape[0]
    blocks = patches.reshape(slots, BLOCK, patches.shape[-1])
    table, stacks, windows = open_pieces(block_counts, send_counts, patch_grids, blocks)
    for group in range(len(GROUPS)):
        for piece in range(len(PIECES)):
            fars = exchange(windows[piece], group)
            if group == len(GROUPS) - 1:
                stacks[piece] = [stacks[piece]] + fars
                continue
            stacks[piece], windows[piece] = turn(table, stacks[piece], fars, group)
    return table, stacks


def dot_nt(a, b):
    return lax.dot_general(a, b, (((1,), (1,)), ((), ())), preferred_element_type=jnp.float32)


def dot_tn(a, b):
    return lax.dot_general(a, b, (((0,), (0,)), ((), ())), preferred_element_type=jnp.float32)


def dot_nn(a, b):
    return lax.dot_general(a, b, (((1,), (0,)), ((), ())), preferred_element_type=jnp.float32)


def image_of_tokens(grid, positions):
    images = grid.shape[1] // 2
    zero = jnp.zeros_like(positions)
    segment, first, span, inside = zero - 1.0, zero, zero + 1.0, zero
    start = jnp.zeros((1, 1), jnp.float32)
    for j in range(images):
        width = grid[:, 2 * j + 1 : 2 * j + 2]
        end = start + grid[:, 2 * j : 2 * j + 1] * width
        member = (positions >= start) & (positions < end)
        segment = jnp.where(member, float(j), segment)
        first = jnp.where(member, start, first)
        span = jnp.where(member, width, span)
        inside = jnp.where(member, 1.0, inside)
        start = end
    offset = (positions - first) * inside
    row = jnp.floor((offset + 0.5) / span)
    return segment, row, offset - row * span, inside


def layer_kernel(
    table_ref,
    *refs,
):
    pieces = len(PIECES)
    group = len(GROUPS) - 1
    each = 1 + len(masks_of(group))
    arrivals = [refs[piece * each : (piece + 1) * each] for piece in range(pieces)]
    (
        levels_ref,
        gain_ref,
        bias_ref,
        w_turned_hbm,
        turn_qkv_hbm,
        b_qkv_ref,
        w_out_hbm,
        turn_out_hbm,
        b_out_ref,
        cot_hbm,
        result_hbm,
        given_hbm,
        kept_hbm,
        x_ref,
        normed_ref,
        mixed_ref,
        grad_ref,
        attended_ref,
        out_grad_ref,
        attn_grad_ref,
        lines_ref,
        seg_row_ref,
        seg_col_ref,
        w_turned_ref,
        turn_qkv_ref,
        w_out_ref,
        turn_out_ref,
        cot_ref,
        result_ref,
        given_ref,
        kept_ref,
        sems,
        raw_sems,
        out_sems,
        *raw_refs,
    ) = refs[pieces * each :]
    balanced = raw_refs[0].shape[0]
    width = x_ref.shape[1]
    inner = w_out_ref.shape[0]
    heads = inner // HEAD
    live_count = table_ref[len(GROUPS) * FIELDS]
    images = 4
    spots = landings(table_ref, group)
    raws = []
    for piece in range(pieces):
        for slot in range(balanced):
            stays = pltpu.make_async_copy(
                arrivals[piece][0].at[slot], raw_refs[piece].at[slot], raw_sems.at[piece]
            )
            raws.append(stays)
            home = jnp.bool_(True)
            for far, (start, total) in zip(arrivals[piece][1:], spots):
                here = (slot >= start) & (slot < start + total)
                home = home & jnp.logical_not(here)
                source = jnp.clip(slot - start, 0, WINDOW - 1)

                @pl.when(here)
                def _():
                    pltpu.make_async_copy(
                        far.at[source], raw_refs[piece].at[slot], raw_sems.at[piece]
                    ).start()

            pl.when(home)(stays.start)
    copies = [
        pltpu.make_async_copy(src, dst, sems.at[i])
        for i, (src, dst) in enumerate(
            (
                (cot_hbm, cot_ref),
                (w_out_hbm, w_out_ref),
                (w_turned_hbm, w_turned_ref),
                (turn_qkv_hbm, turn_qkv_ref),
                (turn_out_hbm, turn_out_ref),
            )
        )
    ]
    for copy in copies:
        copy.start()
    leaving = [
        pltpu.make_async_copy(src, dst, out_sems.at[i])
        for i, (src, dst) in enumerate(
            ((result_ref, result_hbm), (given_ref, given_hbm), (kept_ref, kept_hbm))
        )
    ]

    col = lax.broadcasted_iota(jnp.int32, (BLOCK, 1), 0).astype(jnp.float32)
    lane = lax.broadcasted_iota(jnp.int32, (1, BLOCK), 1).astype(jnp.float32)
    level = lax.broadcasted_iota(jnp.int32, (BLOCK, levels_ref.shape[0]), 1).astype(jnp.float32)
    half = float(levels_ref.shape[0] // 2)

    for raw in raws:
        raw.wait()
    for slot in range(balanced):
        at = slot * BLOCK
        grid = raw_refs[0][slot, PIECES[0] : PIECES[0] + MARK, :BLOCK].astype(jnp.float32)
        grid = grid[0:1, : 2 * images]
        segment, row, column, inside = image_of_tokens(grid, col)
        seg_col_ref[at : at + BLOCK, :] = segment
        seg_row_ref[slot] = jnp.broadcast_to(
            image_of_tokens(grid, lane)[0], (8, BLOCK)
        )
        hot = jnp.where((level == row) | (level == column + half), inside, 0.0)
        emb = dot_nn(hot.astype(jnp.bfloat16), levels_ref[...])
        begin = 0
        for piece, rows in enumerate(PIECES):
            raw = raw_refs[piece][slot, :rows, :].astype(jnp.float32)
            x_ref[at + begin : at + begin + rows, :] = (
                raw + emb[begin : begin + rows, :]
            ).astype(jnp.bfloat16)
            begin += rows
        rows = x_ref[at : at + BLOCK, :].astype(jnp.float32)
        centred = rows - jnp.sum(rows, axis=1, keepdims=True) * (1.0 / width)
        variance = jnp.sum(centred * centred, axis=1, keepdims=True) * (1.0 / width)
        normed_ref[at : at + BLOCK, :] = (
            centred * lax.rsqrt(variance + EPSILON) * gain_ref[...] + bias_ref[...]
        ).astype(jnp.bfloat16)

    copies[0].wait()
    for slot in range(balanced):
        at = slot * BLOCK
        keep = (seg_col_ref[at : at + BLOCK, :] >= 0.0) & (slot < live_count)
        out_grad_ref[at : at + BLOCK, :] = jnp.where(
            keep, cot_ref[at : at + BLOCK, :].astype(jnp.float32), 0.0
        ).astype(jnp.bfloat16)
    copies[1].wait()
    attn_grad_ref[...] = dot_nt(w_out_ref[...], out_grad_ref[...]).astype(jnp.bfloat16)
    copies[2].wait()
    step = 640
    for at in range(0, 3 * inner, step):
        mixed_ref[at : at + step, :] = (
            dot_nt(w_turned_ref[at : at + step, :], normed_ref[...]) + b_qkv_ref[at : at + step, :]
        ).astype(jnp.bfloat16)
    copies[3].wait()
    for at in range(0, width, step):
        mixed_ref[3 * inner + at : 3 * inner + at + step, :] = dot_nt(
            turn_qkv_ref[at : at + step, :], normed_ref[...]
        ).astype(jnp.bfloat16)

    scale = 1.0 / math.sqrt(HEAD)

    def one_slot(slot, carry):
        at = pl.multiple_of(slot * BLOCK, BLOCK)
        span = pl.ds(at, BLOCK)
        same = seg_col_ref[span, :] == seg_row_ref[slot, 0:1, :]
        for head in range(heads):
            h = head * HEAD
            query = mixed_ref[h : h + HEAD, span]
            key = mixed_ref[inner + h : inner + h + HEAD, span]
            value = mixed_ref[2 * inner + h : 2 * inner + h + HEAD, span]
            attn_grad = attn_grad_ref[h : h + HEAD, span]
            scores = jnp.where(same, dot_tn(key, query) * scale, -1e30)
            expo = jnp.exp(scores - jnp.max(scores, axis=0, keepdims=True))
            probs = expo * (1.0 / jnp.sum(expo, axis=0, keepdims=True))
            probs_b = probs.astype(jnp.bfloat16)
            attended_ref[h : h + HEAD, span] = dot_nn(value, probs_b).astype(jnp.bfloat16)
            prob_grad = dot_tn(value, attn_grad)
            grad_ref[2 * inner + h : 2 * inner + h + HEAD, span] = dot_nt(
                attn_grad, probs_b
            ).astype(jnp.bfloat16)
            mean = jnp.sum(prob_grad * probs, axis=0, keepdims=True)
            score_grad = (probs * (prob_grad - mean) * scale).astype(jnp.bfloat16)
            grad_ref[h : h + HEAD, span] = dot_nn(key, score_grad).astype(jnp.bfloat16)
            grad_ref[inner + h : inner + h + HEAD, span] = dot_nt(query, score_grad).astype(
                jnp.bfloat16
            )
        return carry

    lax.fori_loop(0, balanced, one_slot, 0)

    for slot in range(balanced):
        at = slot * BLOCK
        projected = dot_tn(attended_ref[:, at : at + BLOCK], w_out_ref[...]) + b_out_ref[...]
        total = x_ref[at : at + BLOCK, :].astype(jnp.float32) + projected
        result_ref[at : at + BLOCK, :] = jnp.where(slot < live_count, total, 0.0).astype(
            jnp.bfloat16
        )

    leaving[0].start()
    copies[4].wait()
    turned = dot_nn(turn_out_ref[...], attended_ref[...]).astype(jnp.bfloat16)
    chips = given_ref.shape[0]
    pitch = chips + PAD
    qkv_tiles = 3 * inner // 128
    out_tiles = width // 128
    per_rank = width // (2 * chips)
    out_rank = inner // (2 * chips)
    base = 3 * inner
    even = 8 * chips
    for part, target in enumerate((given_ref, kept_ref)):
        row = base + part * per_rank * chips
        eights = mixed_ref[row : row + even, :]
        others = mixed_ref[row + even : row + per_rank * chips, :]
        rest = per_rank - 8
        group = 3
        for tile in range(0, qkv_tiles, group):
            piece = grad_ref[tile * 128 : (tile + group) * 128, :]
            block = dot_nt(eights, piece).astype(jnp.bfloat16)
            side = dot_nt(others, piece)
            for t in range(group):
                target[:, 8 * (tile + t) : 8 * (tile + t) + 8, :] = block[
                    :, t * 128 : (t + 1) * 128
                ].reshape(chips, 8, 128)
                for e in range(rest):
                    line = ((tile + t) * rest + e) * pitch
                    lines_ref[line : line + chips, :] = side[
                        e * chips : (e + 1) * chips, t * 128 : (t + 1) * 128
                    ]
        block = dot_nn(turned[part * out_rank * chips : (part + 1) * out_rank * chips, :], out_grad_ref[...])
        for t in range(out_tiles):
            for e in range(out_rank):
                line = (qkv_tiles * rest + t * out_rank + e) * pitch
                lines_ref[line : line + chips, :] = block[
                    e * chips : (e + 1) * chips, t * 128 : (t + 1) * 128
                ]
        count = qkv_tiles * rest + out_tiles * out_rank

        def one_chip(chip, carry):
            for b in range(count // 8):
                lines = lines_ref[pl.ds(chip + b * 8 * pitch, 8, stride=pitch), :]
                target[chip, 8 * qkv_tiles + 8 * b : 8 * qkv_tiles + 8 * b + 8, :] = lines.astype(
                    jnp.bfloat16
                )
            return carry

        lax.fori_loop(0, chips, one_chip, 0, unroll=8)
        leaving[1 + part].start()
    for copy in leaving:
        copy.wait()


def layer(
    table, stacks, levels, gain, bias, w_turned, turn_qkv, b_qkv, w_out, turn_out, b_out, cotangent
):
    width = cotangent.shape[1]
    tokens = cotangent.shape[0]
    balanced = tokens // BLOCK
    inner = w_out.shape[0]
    chips = lax.axis_size(AXIS) // 2
    lines = (width // (2 * chips) * 3 * inner + inner // (2 * chips) * width) // 128
    any_space = pl.BlockSpec(memory_space=pl.ANY)
    arrived = [array for piece in stacks for array in piece]
    bf16, f32 = jnp.bfloat16, jnp.float32
    return pl.pallas_call(
        layer_kernel,
        out_shape=(
            jax.ShapeDtypeStruct((tokens, width), bf16),
            jax.ShapeDtypeStruct((chips, lines, 128), bf16),
            jax.ShapeDtypeStruct((chips, lines, 128), bf16),
        ),
        in_specs=[SMEM]
        + [any_space] * len(arrived)
        + [VMEM, VMEM, VMEM, any_space, any_space, VMEM, any_space, any_space, VMEM, any_space],
        out_specs=(any_space,) * 3,
        scratch_shapes=[
            pltpu.VMEM((tokens, width), bf16),
            pltpu.VMEM((tokens, width), bf16),
            pltpu.VMEM((3 * inner + width, tokens), bf16),
            pltpu.VMEM((3 * inner, tokens), bf16),
            pltpu.VMEM((inner, tokens), bf16),
            pltpu.VMEM((tokens, width), bf16),
            pltpu.VMEM((inner, tokens), bf16),
            pltpu.VMEM(((lines - 8 * (3 * inner // 128)) * (chips + PAD), 128), f32),
            pltpu.VMEM((balanced, 8, BLOCK), f32),
            pltpu.VMEM((tokens, 1), f32),
            pltpu.VMEM(w_turned.shape, bf16),
            pltpu.VMEM(turn_qkv.shape, bf16),
            pltpu.VMEM(w_out.shape, bf16),
            pltpu.VMEM(turn_out.shape, bf16),
            pltpu.VMEM(cotangent.shape, bf16),
            pltpu.VMEM((tokens, width), bf16),
            pltpu.VMEM((chips, lines, 128), bf16),
            pltpu.VMEM((chips, lines, 128), bf16),
            pltpu.SemaphoreType.DMA((5,)),
            pltpu.SemaphoreType.DMA((len(PIECES),)),
            pltpu.SemaphoreType.DMA((3,)),
        ]
        + [
            pltpu.VMEM((balanced, payload_rows(piece), width), bf16)
            for piece in range(len(PIECES))
        ],
        compiler_params=pltpu.CompilerParams(vmem_limit_bytes=48 * 1024 * 1024),
        name="layer",
    )(
        table,
        *arrived,
        levels,
        gain,
        bias,
        w_turned,
        turn_qkv,
        b_qkv,
        w_out,
        turn_out,
        b_out,
        cotangent,
    )


def turn_over_kernel(w_ref, out_ref):
    for at in range(0, w_ref.shape[1], 128):
        out_ref[at : at + 128, :] = w_ref[:, at : at + 128].T


def turned(w):
    return pl.pallas_call(
        turn_over_kernel,
        out_shape=jax.ShapeDtypeStruct(w.shape[::-1], w.dtype),
        in_specs=[VMEM],
        out_specs=VMEM,
        compiler_params=pltpu.CompilerParams(vmem_limit_bytes=2 * SMALL),
        name="turn_over",
    )(w)


def row_orders(width, inner):
    size = lax.axis_size(AXIS)
    chips = size // 2
    core = lax.axis_index(AXIS) & 1
    cores = jnp.stack([1 - core, core]).astype(jnp.int32)
    chip = jnp.arange(chips, dtype=jnp.int32)
    per, out = width // size, inner // size
    owner = (2 * chip[None, :] + cores[:, None]) * per
    eights = (owner[:, :, None] + jnp.arange(8, dtype=jnp.int32)).reshape(2, -1)
    others = (owner[:, None, :] + jnp.arange(8, per, dtype=jnp.int32)[None, :, None]).reshape(2, -1)
    qkv = jnp.concatenate([eights, others], axis=1).reshape(-1)
    owner = (2 * chip[None, :] + cores[:, None]) * out
    outs = (owner[:, None, :] + jnp.arange(out, dtype=jnp.int32)[None, :, None]).reshape(-1)
    return qkv, outs


def hot_rows(order):
    size = order.shape[0]
    return (order[:, None] == jnp.arange(size, dtype=jnp.int32)[None, :]).astype(jnp.bfloat16)


def chips_with_my_core(size):
    return [[2 * chip + core for chip in range(size // 2)] for core in range(2)]


def spread(given, kept, width, inner):
    size = lax.axis_size(AXIS)
    taken = lax.ppermute(given, AXIS, [(i, i ^ 1) for i in range(size)])
    pair = (kept.astype(jnp.float32) + taken.astype(jnp.float32)).astype(jnp.bfloat16)
    parts = lax.all_to_all(
        pair, AXIS, 0, 0, axis_index_groups=chips_with_my_core(size), tiled=True
    )
    total = jnp.sum(parts.astype(jnp.float32), axis=0)
    tiles, rest, out = 3 * inner // 128, width // size - 8, inner // size
    cuts = (8 * tiles, (8 + rest) * tiles)
    eights = total[: cuts[0]].reshape(tiles, 8, 128).transpose(1, 0, 2).reshape(8, -1)
    others = total[cuts[0] : cuts[1]].reshape(tiles, rest, 128).transpose(1, 0, 2).reshape(rest, -1)
    outs = total[cuts[1] :].reshape(width // 128, out, 128).transpose(1, 0, 2).reshape(out, -1)
    return jnp.concatenate([eights, others], axis=0), outs


def local(
    patches,
    patch_grids,
    block_counts,
    send_counts,
    row_table,
    col_table,
    ln_gain,
    ln_bias,
    w_qkv,
    b_qkv,
    w_out,
    b_out,
    cotangent,
):
    width, inner = cotangent.shape[1], w_out.shape[0]
    qkv_order, out_order = row_orders(width, inner)
    w_turned = turned(w_qkv)
    turn_qkv = hot_rows(qkv_order)
    turn_out = hot_rows(out_order)
    table, stacks = balance(patches, patch_grids, block_counts, send_counts)
    result, given, kept = layer(
        table,
        stacks,
        jnp.concatenate([row_table, col_table], axis=0),
        ln_gain.astype(jnp.float32).reshape(1, -1),
        ln_bias.astype(jnp.float32).reshape(1, -1),
        w_turned,
        turn_qkv,
        b_qkv.astype(jnp.float32).reshape(-1, 1),
        w_out,
        turn_out,
        b_out.astype(jnp.float32).reshape(1, -1),
        cotangent,
    )
    qkv_rows, out_rows = spread(given, kept, width, inner)
    return (result, qkv_rows, out_rows)


def solution(mesh):
    return jax.shard_map(
        local,
        mesh=mesh,
        in_specs=(P(AXIS, None), P(AXIS, None, None)) + (P(),) * 10 + (P(AXIS, None),),
        out_specs=(P(AXIS, None), P(AXIS, None), P(AXIS, None)),
        check_vma=False,
    )
```
